32 devices in a mesh: ep: 8 (over y, x, core), dp: 4 (over z).
Axes of the slice: x: 2, y: 2, z: 4, core: 2. Of those that a mesh axis runs over, the one named last changes fastest.
Arguments:
- resid: bfloat16 [512, 4096], P(('ep', 'dp')), may hold values from -6 to 6
- queries: bfloat16 [512, 8192], P(('ep', 'dp')), may hold values from -4.5 to 4.5
- new_keys: bfloat16 [512, 512], P(('ep', 'dp')), may hold values from -4.5 to 4.5
- new_values: bfloat16 [512, 512], P(('ep', 'dp')), may hold values from -6 to 6
- cache_keys: bfloat16 [512, 128, 512], P(('ep', 'dp')), may hold values from -4.5 to 4.5
- cache_values: bfloat16 [512, 128, 512], P(('ep', 'dp')), may hold values from -6 to 6
- cache_len: int32 [512], P(('ep', 'dp')), may hold values from 1 to 128
- out_proj: bfloat16 [8192, 4096], P('ep'), may hold values from -0.0625 to 0.0625
- norm_gain: float32 [4096], replicated, may hold values from 0.1 to 1.9
- router: bfloat16 [4096, 16], replicated, may hold values from -4 to 4
- expert_ids: int32 [512, 8], P(('ep', 'dp')), may hold values from 0 to 15, all different within a row; in each aligned block of 16 rows (0 to 15, 16 to 31, ...) at most 14 rows name the same one
- gate_slab: bfloat16 [32, 4096, 384], P(('ep', 'dp')), may hold values from -0.09375 to 0.09375
- up_slab: bfloat16 [32, 4096, 384], P(('ep', 'dp')), may hold values from -0.09375 to 0.09375
- down_slab: bfloat16 [32, 384, 4096], P(('ep', 'dp')), may hold values from -0.21875 to 0.21875
Outputs:
- mixed: float32 [512, 4096], P(('ep', 'dp'))
The draws below stay inside these ranges and needn't reach their ends.
Inputs may be any that keep to these rules, and one draw needn't show every extreme that they name: `expert_ids`: each row names 8 different experts; among the rows of one device no expert is named by more than 14 rows.
All inputs are finite; a program needn't handle non-finite values.
Results may differ from the reference program's by a relative error of at most 0.009.
Values may be sent and summed in bfloat16 or wider, within the bound.
A program may use at most 128 MiB of HBM per device.

```python
import math
import jax
import jax.numpy as jnp
import numpy as np
from jax import lax

D = 4096
H = 64
KVH = 4
HD = 128
TOP = 8
FF = 768
TOK_DEV = 16
CACHE = 128
EXPERTS = 16
HF = 384
CAP = 14
TOKENS = 512
N_EP = 8
DEVICES = 32


edge_value = 4.5


def draw_queries(key, part):
    sampled = jnp.clip(jax.random.normal(jax.random.fold_in(key, 1), (TOKENS, H * HD), jnp.float32), -edge_value, edge_value)
    return sampled.astype(jnp.bfloat16)


def draw_cache_keys(key, part):
    sampled = jnp.clip(jax.random.normal(jax.random.fold_in(key, 2), (TOKENS, CACHE, KVH * HD), jnp.float32), -edge_value, edge_value)
    return sampled.astype(jnp.bfloat16)


def draw_router(key, part):
    sampled = jnp.clip(jax.random.normal(jax.random.fold_in(key, 3), (D, EXPERTS), jnp.float32), -4.0, 4.0) / math.sqrt(D)
    return sampled.astype(jnp.bfloat16)


def with_ends(entries, own_key, low, high):
    place = [jax.random.randint(jax.random.fold_in(own_key, axis), (), 0, length) for axis, length in enumerate(entries.shape)]
    main_axis = entries.shape.index(max(entries.shape))
    neighbour = place[:main_axis] + [(place[main_axis] + 1) % entries.shape[main_axis]] + place[main_axis + 1:]
    return entries.at[tuple(place)].set(low).at[tuple(neighbour)].set(high)


def shard_levels(rng, shape, split, least, high):
    loudness, own = 1.0, jax.random.fold_in(rng, 6)
    for axis_at, parts in split:
        steps = jnp.exp(jax.random.uniform(jax.random.fold_in(own, axis_at), (parts,), jnp.float32, least / len(split), high / len(split)))
        loudness = loudness * jnp.repeat(steps, shape[axis_at] // parts).reshape([-1 if axis == axis_at else 1 for axis in range(len(shape))])
    return loudness


def assign_block(rng, own, number, rows, number_of, top, reach, lean):
    order = jax.random.permutation(rng, number_of)
    heavy_load, ordinary = portions_of(number_of, rows * top, reach, lean, True), portions_of(number_of, rows * top, reach, lean, False)
    places = jnp.arange(number_of)

    def named(sizes, offset_by):
        used = int((sizes > 0).sum())
        fixed = max(1, used // 4)
        passed = fixed + (places - fixed + offset_by * (used - fixed)) % max(1, number_of - fixed)
        return jnp.zeros((number_of,), jnp.int32).at[order[jnp.where(places < fixed, places, passed)]].set(jnp.asarray(sizes, jnp.int32))

    sizes = jnp.where(number % 4 == 0, named(heavy_load, number // 4), named(ordinary, number - number // 4 - 1))
    mixed = jax.random.permutation(jax.random.fold_in(own, 3), number_of)
    donor, sink = mixed[0:number_of // 2 * 2:2], mixed[1:number_of // 2 * 2:2]
    margin = jnp.minimum(sizes[donor] - 1, reach - sizes[sink]) // 2
    margin = jnp.where((donor == order[0]) | (sink == order[0]) | (sizes[sink] == 0), 0, jnp.maximum(margin, 0))
    passed = jax.random.randint(jax.random.fold_in(own, 4), (number_of // 2,), 0, 1 << 20) % (margin + 1)
    sizes = sizes.at[donor].add(-passed).at[sink].add(passed)
    labels = jnp.searchsorted(jnp.cumsum(sizes), jnp.arange(rows * top), side="right").astype(jnp.int32)
    listing = labels.reshape(top, rows).T
    listing = listing[jax.random.permutation(jax.random.fold_in(own, 1), rows)]
    offset_by = jax.random.randint(jax.random.fold_in(own, 2), (rows, 1), 0, top)
    return jnp.take_along_axis(listing, (jnp.arange(top)[None, :] + offset_by) % top, axis=1)


def portions_of(count, total, limit, skew, full):
    portions = [(1 << 20) // math.isqrt(rank ** skew) + 1 for rank in range(1, count + 1)]
    largest = limit if full else min(limit, max(-(-total // count), total * portions[0] // sum(portions)))
    least = 1 if total - largest >= count - 1 else 0
    given, spare = [largest] + [least] * (count - 1), total - largest - least * (count - 1)
    while spare > 0:
        movable = [i for i in range(1, count) if given[i] < largest] or [i for i in range(1, count) if given[i] < limit]
        mass, left = sum([portions[i] for i in movable]), spare
        for i in movable:
            addition = min(limit - given[i], max(1, left * portions[i] // mass), spare)
            given[i] = given[i] + addition
            spare = spare - addition
    return np.array(given)


def scatter_about(key, dims, width, reach, cuts=(), held_as=jnp.bfloat16):
    values = width * jax.random.normal(key, dims, jnp.float32)
    if cuts:
        values = values * shard_levels(key, dims, cuts, -0.22, 0.18)
    return jnp.clip(values, -reach, reach).astype(held_as)


def setup_inputs(seed: int = 0) -> dict:
    seeds = jax.random.split(jax.random.key(seed), 15)
    resid = scatter_about(seeds[0], (TOKENS, D), 1.0, 6.0, ((0, 32),))
    queries = draw_queries(jax.random.fold_in(seeds[14], 71), 0)
    new_keys = scatter_about(seeds[2], (TOKENS, KVH * HD), 1.0, 4.5, ((0, 32),))
    new_values = scatter_about(seeds[3], (TOKENS, KVH * HD), 1.0, 6.0, ((0, 32),))
    cache_keys = draw_cache_keys(jax.random.fold_in(seeds[14], 71), 0)
    cache_values = scatter_about(seeds[5], (TOKENS, CACHE, KVH * HD), 1.0, 6.0, ((0, 32),))
    cache_len = with_ends(jax.random.randint(seeds[6], (TOKENS,), 1, CACHE + 1), jax.random.fold_in(seeds[6], 1), 1, CACHE).astype(jnp.int32)
    out_proj = scatter_about(seeds[7], (H * HD, D), (H * HD) ** -0.5, 0.0625, ((0, 8),))
    norm_gain = jnp.clip(1.0 + 0.18 * jax.random.normal(seeds[8], (D,), jnp.float32), 0.1, 1.9)
    router = draw_router(jax.random.fold_in(seeds[14], 71), 0)
    expert_ids_keys = jax.random.split(jax.random.fold_in(seeds[10], 1), TOKENS // TOK_DEV)
    expert_ids_turns = jax.random.permutation(jax.random.fold_in(seeds[10], 3), TOKENS // TOK_DEV)
    expert_ids = jax.vmap(lambda own, number: assign_block(jax.random.fold_in(seeds[10], 2), own, number, TOK_DEV, EXPERTS, TOP, CAP, 2))(expert_ids_keys, expert_ids_turns).reshape((TOKENS, TOP))
    gate_slab = scatter_about(seeds[11], (DEVICES, D, HF), D ** -0.5, 0.09375, ((0, 32),))
    up_slab = scatter_about(seeds[12], (DEVICES, D, HF), D ** -0.5, 0.09375, ((0, 32),))
    down_slab = scatter_about(seeds[13], (DEVICES, HF, D), FF ** -0.5, 0.21875, ((0, 32),))
    return {"resid": resid, "queries": queries, "new_keys": new_keys, "new_values": new_values, "cache_keys": cache_keys, "cache_values": cache_values, "cache_len": cache_len, "out_proj": out_proj, "norm_gain": norm_gain, "router": router, "expert_ids": expert_ids, "gate_slab": gate_slab, "up_slab": up_slab, "down_slab": down_slab}


def attend_block(query_rows, key_new, value_new, key_cache, value_cache, lengths):
    local_rows = query_rows.shape[0]
    cache_span = key_cache.shape[1]
    group_size = H // KVH
    query_heads = query_rows.astype(jnp.float32).reshape(local_rows, KVH, group_size, HD)
    past_keys = key_cache.astype(jnp.float32).reshape(local_rows, cache_span, KVH, HD)
    past_values = value_cache.astype(jnp.float32).reshape(local_rows, cache_span, KVH, HD)
    score_scale = 1.0 / math.sqrt(HD)
    past_scores = jnp.einsum('tgqd,tcgd->tgqc', query_heads, past_keys) * score_scale
    own_scores = jnp.einsum('tgqd,tgd->tgq', query_heads, key_new.astype(jnp.float32).reshape(local_rows, KVH, HD)) * score_scale
    is_valid = lax.broadcasted_iota(jnp.int32, (local_rows, cache_span), 1) < lengths[:, None]
    past_scores = jnp.where(is_valid[:, None, None, :], past_scores, -1e+30)
    peak_score = jnp.maximum(lax.optimization_barrier(jnp.max(past_scores, axis=3)), own_scores)
    past_exp = jnp.exp(past_scores - peak_score[..., None])
    own_exp = jnp.exp(own_scores - peak_score)
    denom_sum = lax.optimization_barrier(jnp.sum(past_exp, axis=3)) + own_exp
    past_weights = lax.optimization_barrier((past_exp / denom_sum[..., None]).astype(jnp.bfloat16))
    own_weights = lax.optimization_barrier((own_exp / denom_sum).astype(jnp.bfloat16))
    blended = jnp.einsum('tgqc,tcgd->tgqd', past_weights.astype(jnp.float32), past_values)
    blended = blended + own_weights.astype(jnp.float32)[..., None] * value_new.astype(jnp.float32).reshape(local_rows, KVH, 1, HD)
    return blended.reshape(local_rows, H * HD).astype(jnp.bfloat16)

def attend_packed(packed):
    return attend_block(*packed)

def blocked(array):
    return array.reshape((DEVICES, TOK_DEV) + array.shape[1:])

def reference(resid, queries, new_keys, new_values, cache_keys, cache_values, cache_len, out_proj, norm_gain, router, expert_ids, gate_slab, up_slab, down_slab):
    packed = (blocked(queries), blocked(new_keys), blocked(new_values), blocked(cache_keys), blocked(cache_values), blocked(cache_len))
    attended = lax.map(attend_packed, packed).reshape(TOKENS, H * HD)
    column_width = H * HD // N_EP
    attn_out = jnp.zeros((TOKENS, D), jnp.float32)
    for shard_index in range(N_EP):
        row_start = shard_index * column_width
        product = jnp.dot(attended[:, row_start:row_start + column_width], out_proj[row_start:row_start + column_width], preferred_element_type=jnp.float32)
        rounded = lax.optimization_barrier(product.astype(jnp.bfloat16))
        attn_out = attn_out + rounded.astype(jnp.float32)
    hidden = resid.astype(jnp.float32) + attn_out
    meansq = lax.optimization_barrier(jnp.mean(hidden * hidden, axis=1, keepdims=True))
    normed = (hidden * lax.rsqrt(jnp.maximum(meansq, 0.25)) * norm_gain).astype(jnp.bfloat16)
    logits = jnp.dot(normed, router, preferred_element_type=jnp.float32)
    chosen = jnp.take_along_axis(logits, expert_ids.astype(jnp.int32), axis=1)
    peak_logit = lax.optimization_barrier(jnp.max(chosen, axis=1, keepdims=True))
    exp_logit = jnp.exp(chosen - peak_logit)
    gate_probs = lax.optimization_barrier((exp_logit / lax.optimization_barrier(jnp.sum(exp_logit, axis=1, keepdims=True))).astype(jnp.bfloat16))
    flat_ids = expert_ids.reshape(-1).astype(jnp.int32)
    token_of = (jnp.arange(TOKENS * TOP, dtype=jnp.int32) // TOP).astype(jnp.int32)
    onehot = (flat_ids[:, None] == jnp.arange(EXPERTS, dtype=jnp.int32)[None, :]).astype(jnp.int32)
    earlier = jnp.cumsum(onehot, axis=0).astype(jnp.int32) - onehot
    ranking = lax.optimization_barrier(jnp.sum(earlier * onehot, axis=1)).astype(jnp.int32)
    row_depth = DEVICES * CAP
    row_table = jnp.zeros((EXPERTS, row_depth), jnp.int32).at[flat_ids, ranking].set(token_of)

    def run_expert(expert):
        rows_in = jnp.take(normed, row_table[expert], axis=0)
        gate_full = jnp.concatenate((gate_slab[2 * expert], gate_slab[2 * expert + 1]), axis=1)
        up_full = jnp.concatenate((up_slab[2 * expert], up_slab[2 * expert + 1]), axis=1)
        down_full = jnp.concatenate((down_slab[2 * expert], down_slab[2 * expert + 1]), axis=0)
        gate_val = jnp.dot(rows_in, gate_full, preferred_element_type=jnp.float32)
        up_val = jnp.dot(rows_in, up_full, preferred_element_type=jnp.float32)
        activated = (jax.nn.silu(gate_val) * up_val).astype(jnp.bfloat16)
        return jnp.dot(activated, down_full, preferred_element_type=jnp.float32).astype(jnp.bfloat16)
    produced = lax.map(run_expert, jnp.arange(EXPERTS, dtype=jnp.int32))
    picked = produced[flat_ids, ranking].reshape(TOKENS, TOP, D)
    expert_mix = jnp.einsum('tk,tkd->td', gate_probs.astype(jnp.float32), picked.astype(jnp.float32))
    return hidden + expert_mix
```

```python
import math

import jax
import jax.numpy as jnp
from jax import lax
from jax.sharding import PartitionSpec as P

D = 4096
H = 64
KVH = 4
HD = 128
TOP = 8


def attend(queries, new_keys, new_values, cache_keys, cache_values, cache_len):
    local_rows = queries.shape[0]
    cache_span = cache_keys.shape[1]
    group_size = H // KVH
    query_heads = queries.reshape(local_rows, KVH, group_size, HD)
    past_keys = cache_keys.reshape(local_rows, cache_span, KVH, HD)
    past_values = cache_values.reshape(local_rows, cache_span, KVH, HD)
    score_scale = 1.0 / math.sqrt(HD)
    past_scores = (
        jnp.einsum("tgqd,tcgd->tgqc", query_heads, past_keys, preferred_element_type=jnp.float32)
        * score_scale
    )
    own_scores = (
        jnp.einsum(
            "tgqd,tgd->tgq",
            query_heads,
            new_keys.reshape(local_rows, KVH, HD),
            preferred_element_type=jnp.float32,
        )
        * score_scale
    )
    is_valid = lax.broadcasted_iota(jnp.int32, (local_rows, cache_span), 1) < cache_len[:, None]
    past_scores = jnp.where(is_valid[:, None, None, :], past_scores, -1e30)
    peak_score = jnp.maximum(jnp.max(past_scores, axis=3), own_scores)
    past_exp = jnp.exp(past_scores - peak_score[..., None])
    own_exp = jnp.exp(own_scores - peak_score)
    denom_sum = jnp.sum(past_exp, axis=3) + own_exp
    past_weights = (past_exp / denom_sum[..., None]).astype(jnp.bfloat16)
    own_weights = (own_exp / denom_sum).astype(jnp.bfloat16)
    blended = jnp.einsum(
        "tgqc,tcgd->tgqd", past_weights, past_values, preferred_element_type=jnp.float32
    )
    blended = blended + own_weights.astype(jnp.float32)[..., None] * new_values.reshape(
        local_rows, KVH, 1, HD
    ).astype(jnp.float32)
    return blended.reshape(local_rows, H * HD).astype(jnp.bfloat16)


def local(
    resid,
    queries,
    new_keys,
    new_values,
    cache_keys,
    cache_values,
    cache_len,
    out_proj,
    norm_gain,
    router,
    expert_ids,
    gate_slab,
    up_slab,
    down_slab,
):
    local_rows = resid.shape[0]
    attended = attend(queries, new_keys, new_values, cache_keys, cache_values, cache_len)
    regrouped = lax.all_to_all(attended, "ep", split_axis=1, concat_axis=0, tiled=True)
    attn_out = lax.psum_scatter(
        jnp.dot(regrouped, out_proj, preferred_element_type=jnp.float32).astype(jnp.bfloat16),
        "ep",
        scatter_dimension=0,
        tiled=True,
    ).astype(jnp.float32)
    hidden = resid.astype(jnp.float32) + attn_out
    meansq = jnp.mean(hidden * hidden, axis=1, keepdims=True)
    normed = (hidden * lax.rsqrt(jnp.maximum(meansq, 0.25)) * norm_gain).astype(jnp.bfloat16)
    logits = jnp.dot(normed, router, preferred_element_type=jnp.float32)
    experts = router.shape[1]
    labels = jnp.arange(experts, dtype=jnp.int32)
    onehot = expert_ids[:, :, None] == labels[None, None, :]
    chosen = jnp.sum(jnp.where(onehot, logits[:, None, :], 0.0), axis=2)
    peak_logit = jnp.max(chosen, axis=1, keepdims=True)
    exp_logit = jnp.exp(chosen - peak_logit)
    gate_probs = (exp_logit / jnp.sum(exp_logit, axis=1, keepdims=True)).astype(jnp.bfloat16)
    weights = jnp.sum(
        jnp.where(onehot, gate_probs.astype(jnp.float32)[:, :, None], 0.0), axis=1
    ).astype(jnp.bfloat16)
    packed = jnp.concatenate((normed, jnp.pad(weights, ((0, 0), (0, (-experts) % 128)))), axis=1)
    gathered = lax.all_gather(packed, ("ep", "dp"), axis=0, tiled=True)
    expert = (lax.axis_index("ep") * lax.axis_size("dp") + lax.axis_index("dp")) // 2
    own = jnp.sum(
        jnp.where(labels[None, :] == expert, gathered[:, D : D + experts].astype(jnp.float32), 0.0),
        axis=1,
        keepdims=True,
    )
    rows = gathered[:, :D]
    gate_val = jnp.dot(rows, gate_slab[0], preferred_element_type=jnp.float32)
    up_val = jnp.dot(rows, up_slab[0], preferred_element_type=jnp.float32)
    activated = (jax.nn.silu(gate_val) * up_val * own).astype(jnp.bfloat16)
    partial = jnp.dot(activated, down_slab[0], preferred_element_type=jnp.float32)
    expert_mix = lax.psum_scatter(
        partial.astype(jnp.bfloat16), ("ep", "dp"), scatter_dimension=0, tiled=True
    )
    return hidden + expert_mix.astype(jnp.float32)


def solution(mesh):
    in_specs = (
        P(("ep", "dp"), None),
        P(("ep", "dp"), None),
        P(("ep", "dp"), None),
        P(("ep", "dp"), None),
        P(("ep", "dp"), None, None),
        P(("ep", "dp"), None, None),
        P(("ep", "dp")),
        P("ep", None),
        P(),
        P(),
        P(("ep", "dp"), None),
        P(("ep", "dp"), None, None),
        P(("ep", "dp"), None, None),
        P(("ep", "dp"), None, None),
    )
    out_specs = P(("ep", "dp"), None)
    return jax.shard_map(local, mesh=mesh, in_specs=in_specs, out_specs=out_specs, check_vma=False)
```

```python
import math

import jax
import jax.numpy as jnp
from jax import lax
from jax.experimental import pallas as pl
from jax.experimental.pallas import tpu as pltpu
from jax.sharding import PartitionSpec as P

D = 4096
H = 64
KVH = 4
HD = 128
TOP = 8


def attend(queries, new_keys, new_values, cache_keys, cache_values, cache_len):
    local_rows = queries.shape[0]
    cache_span = cache_keys.shape[1]
    group_size = H // KVH
    query_heads = queries.reshape(local_rows, KVH, group_size, HD)
    past_keys = cache_keys.reshape(local_rows, cache_span, KVH, HD)
    past_values = cache_values.reshape(local_rows, cache_span, KVH, HD)
    score_scale = 1.0 / math.sqrt(HD)
    past_scores = (
        jnp.einsum("tgqd,tcgd->tgqc", query_heads, past_keys, preferred_element_type=jnp.float32)
        * score_scale
    )
    own_scores = (
        jnp.einsum(
            "tgqd,tgd->tgq",
            query_heads,
            new_keys.reshape(local_rows, KVH, HD),
            preferred_element_type=jnp.float32,
        )
        * score_scale
    )
    is_valid = lax.broadcasted_iota(jnp.int32, (local_rows, cache_span), 1) < cache_len[:, None]
    past_scores = jnp.where(is_valid[:, None, None, :], past_scores, -1e30)
    peak_score = jnp.maximum(jnp.max(past_scores, axis=3), own_scores)
    past_exp = jnp.exp(past_scores - peak_score[..., None])
    own_exp = jnp.exp(own_scores - peak_score)
    denom_sum = jnp.sum(past_exp, axis=3) + own_exp
    past_weights = (past_exp / denom_sum[..., None]).astype(jnp.bfloat16)
    own_weights = (own_exp / denom_sum).astype(jnp.bfloat16)
    blended = jnp.einsum(
        "tgqc,tcgd->tgqd", past_weights, past_values, preferred_element_type=jnp.float32
    )
    blended = blended + own_weights.astype(jnp.float32)[..., None] * new_values.reshape(
        local_rows, KVH, 1, HD
    ).astype(jnp.float32)
    return blended.reshape(local_rows, H * HD).astype(jnp.bfloat16)


MESH = pl.DeviceIdType.MESH
VMEM_LIMIT = 66_000_000


class Place:
    def __init__(self, side, depth):
        self.side, self.depth = side, depth
        ep = lax.axis_index("ep")
        self.ep = ep
        self.core = lax.rem(ep, 2)
        self.x = lax.rem(ep // 2, side)
        self.y = ep // (2 * side)
        self.z = lax.axis_index("dp")

    def at(self, dy=0, dx=0, dz=0, flip=False):
        y, x = self.line(dy, dx)
        z = lax.rem(self.z + dz, self.depth) if dz else self.z
        core = 1 - self.core if flip else self.core
        return ((y * self.side + x) * 2 + core, z)

    def line(self, dy, dx):
        return lax.rem(self.y + dy, self.side), lax.rem(self.x + dx, self.side)


def greet(devices):
    barrier = pltpu.get_barrier_semaphore()
    for device in devices:
        pl.semaphore_signal(barrier, inc=1, device_id=device, device_id_type=MESH)
    pl.semaphore_wait(barrier, len(devices))


def remote(src, dst, send, recv, device):
    return pltpu.make_async_remote_copy(
        src_ref=src, dst_ref=dst, send_sem=send, recv_sem=recv, device_id=device, device_id_type=MESH
    )


def slices_of(width, extra=0):
    step = 512
    cuts = [[start, step] for start in range(0, width, step)]
    cuts[-1][1] += extra
    return cuts


def reduce_shapes(side, depth, rows, width):
    n = width // 512
    lines = side * side
    bf, dma = jnp.bfloat16, pltpu.SemaphoreType.DMA
    tall = depth * rows
    return [
        pltpu.VMEM((side, side, tall, width), bf),
        pltpu.VMEM((side, side, tall, width), bf),
        pltpu.VMEM((side - 1, side, tall, width), bf),
        pltpu.VMEM((side, tall, width), bf),
        pltpu.VMEM((side - 1, tall, width), bf),
        pltpu.VMEM((depth, rows, width), bf),
        pltpu.VMEM((max(depth - 1, 1), rows, width), bf),
        dma((n, 2)),
        dma((n, side, side, 2)),
        dma((n, side, 2)),
        dma((n, depth, 2)),
    ]


def reduce_scatter(here, rows, width, produce, finish, part, scratch):
    in1, sum1, in2, sum2, in3, sum3, in4, sem1, sem2, sem3, sem4 = scratch
    side, depth = here.side, here.depth
    cuts = slices_of(width)
    sends = []

    def core_copy(s):
        start, size = cuts[s]
        cols = pl.ds(start, size)
        return remote(
            part.at[:, :, 1 - here.core, :, cols],
            in1.at[:, :, :, cols],
            sem1.at[s, 0],
            sem1.at[s, 1],
            here.at(flip=True),
        )

    def offsets(s, a, b):
        return (a, b) if s % 2 == 0 else (b, a)

    def first_copy(s, ja, kb, sending):
        cols = pl.ds(*cuts[s])
        slot = side - ja - 1
        y, x = here.line(*offsets(s, ja, kb))
        return remote(
            sum1.at[y, x, :, cols],
            in2.at[slot, kb, :, cols],
            sem2.at[s, ja, kb, 0],
            sem2.at[s, side - ja if sending else ja, kb, 1],
            here.at(*offsets(s, ja, 0)),
        )

    def second_copy(s, kb, sending):
        cols = pl.ds(*cuts[s])
        return remote(
            sum2.at[kb, :, cols],
            in3.at[side - kb - 1, :, cols],
            sem3.at[s, kb, 0],
            sem3.at[s, side - kb if sending else kb, 1],
            here.at(*offsets(s, 0, kb)),
        )

    def depth_copy(s, jz, sending):
        cols = pl.ds(*cuts[s])
        return remote(
            sum3.at[lax.rem(here.z + jz, depth), :, cols],
            in4.at[depth - jz - 1, :, cols],
            sem4.at[s, jz, 0],
            sem4.at[s, depth - jz if sending else jz, 1],
            here.at(0, 0, jz),
        )

    def go(copy):
        copy.start()
        sends.append(copy)

    def wide(value):
        return value.astype(jnp.float32)

    def phase0(s):
        cols = pl.ds(*cuts[s])
        value = produce(s, cols)
        part[:, :, :, :, cols] = value.astype(jnp.bfloat16).reshape(
            side, side, 2, depth * rows, cuts[s][1]
        )
        go(core_copy(s))

    def phase1(s):
        cols = pl.ds(*cuts[s])
        core_copy(s).wait_recv()
        for a in list(range(1, side)) + [0]:
            for b in list(range(1, side)) + [0]:
                y, x = here.line(*offsets(s, a, b))
                total = wide(part[y, x, here.core, :, cols]) + wide(in1[y, x, :, cols])
                sum1[y, x, :, cols] = total.astype(jnp.bfloat16)
                if a:
                    go(first_copy(s, a, b, True))

    def phase2(s):
        cols = pl.ds(*cuts[s])
        for b in list(range(1, side)) + [0]:
            y, x = here.line(*offsets(s, 0, b))
            total = wide(sum1[y, x, :, cols])
            for a in range(1, side):
                first_copy(s, a, b, False).wait_recv()
                total = total + wide(in2[a - 1, b, :, cols])
            sum2[b, :, cols] = total.astype(jnp.bfloat16)
            if b:
                go(second_copy(s, b, True))

    def phase3(s):
        cols = pl.ds(*cuts[s])
        total = wide(sum2[0, :, cols])
        for b in range(1, side):
            second_copy(s, b, False).wait_recv()
            total = total + wide(in3[b - 1, :, cols])
        if depth == 1:
            finish(s, cols, total)
            return
        sum3[:, :, cols] = total.astype(jnp.bfloat16).reshape(depth, rows, cuts[s][1])
        for jz in range(1, depth):
            go(depth_copy(s, jz, True))

    def phase4(s):
        if depth == 1:
            return
        cols = pl.ds(*cuts[s])
        total = wide(sum3[here.z, :, cols])
        for jz in range(1, depth):
            depth_copy(s, jz, False).wait_recv()
            total = total + wide(in4[jz - 1, :, cols])
        finish(s, cols, total)

    phases = ((phase0, 0), (phase1, 1), (phase2, 3), (phase3, 5), (phase4, 7))
    for step in range(len(cuts) + phases[-1][1]):
        for phase, lag in phases:
            if 0 <= step - lag < len(cuts):
                phase(step - lag)
    for copy in sends:
        copy.wait_send()


def plane_of(here):
    side = here.side
    return (
        [here.at(flip=True)]
        + [here.at(dy=j) for j in range(1, side)]
        + [here.at(dx=j) for j in range(1, side)]
    )


def projection_kernel(side, attended, weight_hbm, resid, hidden, weight, regrouped, part, wsem, ssem, rsem, *scratch):
    here = Place(side, 1)
    rows = attended.shape[0]
    count = 2 * side * side
    width = attended.shape[1] // count
    z = lax.axis_index("dp")
    load = pltpu.make_async_copy(weight_hbm, weight, wsem)
    load.start()

    def peer(j):
        return lax.rem(here.ep + j, count)

    greet([(peer(j), z) for j in range(1, count)])

    def piece(index):
        return attended.at[:, pl.ds(pl.multiple_of(index * width, 128), width)]

    def exchange(j, sending):
        return remote(
            piece(peer(j)),
            regrouped.at[here.ep],
            ssem.at[j],
            rsem.at[count - j if sending else j],
            (peer(j), z),
        )

    for j in range(1, count):
        exchange(j, True).start()
    regrouped[here.ep] = attended[:, pl.ds(pl.multiple_of(here.ep * width, 128), width)]
    load.wait()
    for j in range(1, count):
        remote(
            piece(peer(j)), regrouped.at[peer(j)], ssem.at[j], rsem.at[j], (peer(j), z)
        ).wait_recv()

    def produce(s, cols):
        left = regrouped[...].reshape(count * rows, width)
        return jnp.dot(left, weight[:, cols], preferred_element_type=jnp.float32)

    def finish(s, cols, total):
        hidden[:, cols] = resid[:, cols].astype(jnp.float32) + total

    reduce_scatter(here, rows, hidden.shape[1], produce, finish, part, scratch)
    for j in range(1, count):
        exchange(j, True).wait_send()


def project(side, attended, out_proj, resid):
    rows, width = resid.shape
    count = 2 * side * side
    dma = pltpu.SemaphoreType.DMA
    return pl.pallas_call(
        lambda *refs: projection_kernel(side, *refs),
        out_shape=jax.ShapeDtypeStruct((rows, width), jnp.float32),
        in_specs=[
            pl.BlockSpec(memory_space=pltpu.VMEM),
            pl.BlockSpec(memory_space=pl.ANY),
            pl.BlockSpec(memory_space=pltpu.VMEM),
        ],
        out_specs=pl.BlockSpec(memory_space=pltpu.VMEM),
        scratch_shapes=[
            pltpu.VMEM(out_proj.shape, jnp.bfloat16),
            pltpu.VMEM((count, rows, attended.shape[1] // count), jnp.bfloat16),
            pltpu.VMEM((side, side, 2, rows, width), jnp.bfloat16),
            dma(()),
            dma((count,)),
            dma((count,)),
        ]
        + reduce_shapes(side, 1, rows, width),
        compiler_params=pltpu.CompilerParams(
            collective_id=0, has_side_effects=True, vmem_limit_bytes=VMEM_LIMIT
        ),
    )(attended, out_proj, resid)


def all_gather(here, own, held, zsem, lsem, csem, send_sem, copy_sem):
    side, depth = here.side, here.depth
    width = D
    cuts = slices_of(width, own.shape[1] - width)
    sends = []
    rows = own.shape[0]

    def rows_of(z):
        return pl.ds(pl.multiple_of(z * rows, rows), rows)

    local_copy = pltpu.make_async_copy(own, held.at[here.y, here.x, here.core, rows_of(here.z)], copy_sem)
    local_copy.start()

    def go(copy):
        copy.start()
        sends.append(copy)

    def depth_copy(s, j, sending):
        cols = pl.ds(*cuts[s])
        z = here.z if sending else lax.rem(here.z + j, depth)
        return remote(
            own.at[:, cols],
            held.at[here.y, here.x, here.core, rows_of(z), cols],
            zsem.at[s, j, 0],
            zsem.at[s, depth - j if sending else j, 1],
            here.at(0, 0, j),
        )

    def line_ref(s, ky, kx, core):
        y, x = here.line(ky, kx)
        return held.at[y, x, core, :, pl.ds(*cuts[s])]

    def plane_send(s, ky, kx, jy, jx):
        ref = line_ref(s, ky, kx, here.core)
        go(
            remote(
                ref,
                ref,
                send_sem.at[s, ky, kx, jy, jx],
                lsem.at[s, (ky - jy) % side, (kx - jx) % side],
                here.at(jy, jx),
            )
        )

    def core_send(s, ky, kx):
        ref = line_ref(s, ky, kx, here.core)
        go(remote(ref, ref, csem.at[s, ky, kx, 0], csem.at[s, ky, kx, 1], here.at(flip=True)))

    def plane_wait(s, ky, kx):
        ref = line_ref(s, ky, kx, here.core)
        remote(ref, ref, send_sem.at[s, 0, 0, 0, 0], lsem.at[s, ky, kx], here.at(flip=True)).wait_recv()

    def core_wait(s, ky, kx):
        ref = line_ref(s, ky, kx, 1 - here.core)
        remote(ref, ref, csem.at[s, ky, kx, 0], csem.at[s, ky, kx, 1], here.at(flip=True)).wait_recv()

    def turn(s, a, b):
        return (a, b) if s % 2 == 0 else (b, a)

    def phase1(s):
        for j in range(1, depth):
            depth_copy(s, j, False).wait_recv()
        for j in range(1, side):
            plane_send(s, 0, 0, *turn(s, j, 0))
            plane_send(s, 0, 0, *turn(s, 0, j))
        core_send(s, 0, 0)

    def phase2(s):
        for k in range(1, side):
            plane_wait(s, *turn(s, k, 0))
            for j in range(1, side):
                plane_send(s, *turn(s, k, 0), *turn(s, 0, j))
            core_send(s, *turn(s, k, 0))

    def phase3(s):
        for b in range(1, side):
            for a in range(side):
                plane_wait(s, *turn(s, a, b))
                core_send(s, *turn(s, a, b))

    for s in range(len(cuts)):
        for j in range(1, depth):
            go(depth_copy(s, j, True))
    local_copy.wait()
    phases = ((phase1, 0), (phase2, 2), (phase3, 4))
    for step in range(len(cuts) + phases[-1][1]):
        for phase, lag in phases:
            if 0 <= step - lag < len(cuts):
                phase(step - lag)
    for s in range(len(cuts)):
        for a in range(side):
            for b in range(side):
                core_wait(s, a, b)
    for copy in sends:
        copy.wait_send()


def expert_kernel(
    side, depth, experts, own, hidden, gate_hbm, up_hbm, down_hbm, mixed,
    gate, up, down, held, act, wsem, zsem, lsem, csem, send_sem, copy_sem, *scratch
):
    here = Place(side, depth)
    rows = own.shape[0]
    loads = [
        pltpu.make_async_copy(src.at[0], dst, wsem.at[i])
        for i, (src, dst) in enumerate(((gate_hbm, gate), (up_hbm, up), (down_hbm, down)))
    ]
    for load in loads:
        load.start()
    greet(plane_of(here) + [here.at(0, 0, j) for j in range(1, depth)])
    all_gather(here, own, held, zsem, lsem, csem, send_sem, copy_sem)
    for load in loads:
        load.wait()
    expert = (here.ep * depth + here.z) // 2
    group = 2 * depth * rows

    def block(i, carry):
        y, x = i // side, lax.rem(i, side)
        all_cols = held[y, x].reshape(group, held.shape[-1])
        row = all_cols[:, :D]
        lane = lax.broadcasted_iota(jnp.int32, (group, held.shape[-1] - D), 1)
        weight = jnp.sum(
            jnp.where(lane == expert, all_cols[:, D:].astype(jnp.float32), 0.0), axis=1, keepdims=True
        )
        gate_val = jnp.dot(row, gate[...], preferred_element_type=jnp.float32)
        up_val = jnp.dot(row, up[...], preferred_element_type=jnp.float32)
        value = gate_val / (1.0 + jnp.exp(-gate_val)) * up_val * weight
        act[pl.ds(pl.multiple_of(i * group, group), group), :] = value.astype(jnp.bfloat16)
        return carry

    lax.fori_loop(0, side * side, block, 0)

    def produce(s, cols):
        return jnp.dot(act[...], down[:, cols], preferred_element_type=jnp.float32)

    def finish(s, cols, total):
        mixed[:, cols] = hidden[:, cols] + total

    reduce_scatter(here, rows, mixed.shape[1], produce, finish, held, scratch)


def run_experts(side, depth, experts, packed, hidden, gate_slab, up_slab, down_slab):
    rows, width = hidden.shape
    n = width // 512
    dma = pltpu.SemaphoreType.DMA
    count = 2 * side * side * depth
    vmem, anywhere = pl.BlockSpec(memory_space=pltpu.VMEM), pl.BlockSpec(memory_space=pl.ANY)
    return pl.pallas_call(
        lambda *refs: expert_kernel(side, depth, experts, *refs),
        out_shape=jax.ShapeDtypeStruct((rows, width), jnp.float32),
        in_specs=[vmem, vmem, anywhere, anywhere, anywhere],
        out_specs=vmem,
        scratch_shapes=[
            pltpu.VMEM(gate_slab.shape[1:], jnp.bfloat16),
            pltpu.VMEM(up_slab.shape[1:], jnp.bfloat16),
            pltpu.VMEM(down_slab.shape[1:], jnp.bfloat16),
            pltpu.VMEM((side, side, 2, depth * rows, packed.shape[1]), jnp.bfloat16),
            pltpu.VMEM((count * rows, gate_slab.shape[2]), jnp.bfloat16),
            dma((3,)),
            dma((n, depth, 2)),
            dma((n, side, side)),
            dma((n, side, side, 2)),
            dma((n, side, side, side, side)),
            dma(()),
        ]
        + reduce_shapes(side, depth, rows, width),
        compiler_params=pltpu.CompilerParams(
            collective_id=1, has_side_effects=True, vmem_limit_bytes=VMEM_LIMIT
        ),
    )(packed, hidden, gate_slab, up_slab, down_slab)


def local(
    resid,
    queries,
    new_keys,
    new_values,
    cache_keys,
    cache_values,
    cache_len,
    out_proj,
    norm_gain,
    router,
    expert_ids,
    gate_slab,
    up_slab,
    down_slab,
):
    attended = attend(queries, new_keys, new_values, cache_keys, cache_values, cache_len)
    side = math.isqrt(lax.axis_size("ep") // 2)
    depth = lax.axis_size("dp")
    hidden = project(side, attended, out_proj, resid)
    meansq = jnp.mean(hidden * hidden, axis=1, keepdims=True)
    normed = (hidden * lax.rsqrt(jnp.maximum(meansq, 0.25)) * norm_gain).astype(jnp.bfloat16)
    logits = jnp.dot(normed, router, preferred_element_type=jnp.float32)
    experts = router.shape[1]
    labels = jnp.arange(experts, dtype=jnp.int32)
    onehot = expert_ids[:, :, None] == labels[None, None, :]
    chosen = jnp.sum(jnp.where(onehot, logits[:, None, :], 0.0), axis=2)
    peak_logit = jnp.max(chosen, axis=1, keepdims=True)
    exp_logit = jnp.exp(chosen - peak_logit)
    gate_probs = (exp_logit / jnp.sum(exp_logit, axis=1, keepdims=True)).astype(jnp.bfloat16)
    weights = jnp.sum(
        jnp.where(onehot, gate_probs.astype(jnp.float32)[:, :, None], 0.0), axis=1
    ).astype(jnp.bfloat16)
    packed = jnp.concatenate((normed, jnp.pad(weights, ((0, 0), (0, (-experts) % 128)))), axis=1)
    return run_experts(side, depth, experts, packed, hidden, gate_slab, up_slab, down_slab)


def solution(mesh):
    in_specs = (
        P(("ep", "dp"), None),
        P(("ep", "dp"), None),
        P(("ep", "dp"), None),
        P(("ep", "dp"), None),
        P(("ep", "dp"), None, None),
        P(("ep", "dp"), None, None),
        P(("ep", "dp")),
        P("ep", None),
        P(),
        P(),
        P(("ep", "dp"), None),
        P(("ep", "dp"), None, None),
        P(("ep", "dp"), None, None),
        P(("ep", "dp"), None, None),
    )
    out_specs = P(("ep", "dp"), None)
    return jax.shard_map(local, mesh=mesh, in_specs=in_specs, out_specs=out_specs, check_vma=False)
```

```python
import math

import jax
import jax.numpy as jnp
from jax import lax
from jax.experimental import pallas as pl
from jax.experimental.pallas import tpu as pltpu
from jax.sharding import PartitionSpec as P

D = 4096
H = 64
KVH = 4
HD = 128
TOP = 8


def attend(queries, new_keys, new_values, cache_keys, cache_values, cache_len):
    local_rows = queries.shape[0]
    cache_span = cache_keys.shape[1]
    group_size = H // KVH
    query_heads = queries.reshape(local_rows, KVH, group_size, HD)
    past_keys = cache_keys.reshape(local_rows, cache_span, KVH, HD)
    past_values = cache_values.reshape(local_rows, cache_span, KVH, HD)
    score_scale = 1.0 / math.sqrt(HD)
    past_scores = (
        jnp.einsum("tgqd,tcgd->tgqc", query_heads, past_keys, preferred_element_type=jnp.float32)
        * score_scale
    )
    own_scores = (
        jnp.einsum(
            "tgqd,tgd->tgq",
            query_heads,
            new_keys.reshape(local_rows, KVH, HD),
            preferred_element_type=jnp.float32,
        )
        * score_scale
    )
    is_valid = lax.broadcasted_iota(jnp.int32, (local_rows, cache_span), 1) < cache_len[:, None]
    past_scores = jnp.where(is_valid[:, None, None, :], past_scores, -1e30)
    peak_score = jnp.maximum(jnp.max(past_scores, axis=3), own_scores)
    past_exp = jnp.exp(past_scores - peak_score[..., None])
    own_exp = jnp.exp(own_scores - peak_score)
    denom_sum = jnp.sum(past_exp, axis=3) + own_exp
    past_weights = (past_exp / denom_sum[..., None]).astype(jnp.bfloat16)
    own_weights = (own_exp / denom_sum).astype(jnp.bfloat16)
    blended = jnp.einsum(
        "tgqc,tcgd->tgqd", past_weights, past_values, preferred_element_type=jnp.float32
    )
    blended = blended + own_weights.astype(jnp.float32)[..., None] * new_values.reshape(
        local_rows, KVH, 1, HD
    ).astype(jnp.float32)
    return blended.reshape(local_rows, H * HD).astype(jnp.bfloat16)


MESH = pl.DeviceIdType.MESH
VMEM_LIMIT = 66_000_000


class Place:
    def __init__(self, side, depth):
        self.side, self.depth = side, depth
        ep = lax.axis_index("ep")
        self.ep = ep
        self.core = lax.rem(ep, 2)
        self.x = lax.rem(ep // 2, side)
        self.y = ep // (2 * side)
        self.z = lax.axis_index("dp")

    def at(self, dy=0, dx=0, dz=0, flip=False):
        y, x = self.line(dy, dx)
        z = lax.rem(self.z + dz, self.depth) if dz else self.z
        core = 1 - self.core if flip else self.core
        return ((y * self.side + x) * 2 + core, z)

    def line(self, dy, dx):
        return lax.rem(self.y + dy, self.side), lax.rem(self.x + dx, self.side)


def greet(devices):
    barrier = pltpu.get_barrier_semaphore()
    for device in devices:
        pl.semaphore_signal(barrier, inc=1, device_id=device, device_id_type=MESH)
    pl.semaphore_wait(barrier, len(devices))


def remote(src, dst, send, recv, device):
    return pltpu.make_async_remote_copy(
        src_ref=src, dst_ref=dst, send_sem=send, recv_sem=recv, device_id=device, device_id_type=MESH
    )


def slices_of(width, extra=0):
    step = 512
    cuts = [[start, step] for start in range(0, width, step)]
    cuts[-1][1] += extra
    return cuts


def reduce_shapes(side, depth, rows, width):
    n = width // 512
    lines = side * side
    bf, dma = jnp.bfloat16, pltpu.SemaphoreType.DMA
    tall = depth * rows
    return [
        pltpu.VMEM((side, side, tall, width), bf),
        pltpu.VMEM((side - 1, side, tall, width), bf),
        pltpu.VMEM((side, tall, width), bf),
        pltpu.VMEM((side - 1, tall, width), bf),
        pltpu.VMEM((depth, rows, width), bf),
        pltpu.VMEM((max(depth - 1, 1), rows, width), bf),
        dma((n, 2)),
        dma((n, side, side, 2)),
        dma((n, side, 2)),
        dma((n, depth, 2)),
    ]


def reduce_scatter(here, rows, width, produce, finish, lags, part, scratch):
    in1, in2, sum2, in3, sum3, in4, sem1, sem2, sem3, sem4 = scratch
    side, depth = here.side, here.depth
    cuts = slices_of(width)
    sends = []

    def core_copy(s):
        start, size = cuts[s]
        cols = pl.ds(start, size)
        return remote(
            part.at[:, :, 1 - here.core, :, cols],
            in1.at[:, :, :, cols],
            sem1.at[s, 0],
            sem1.at[s, 1],
            here.at(flip=True),
        )

    def offsets(s, a, b):
        return (a, b) if s % 2 == 0 else (b, a)

    def first_copy(s, ja, kb, sending):
        cols = pl.ds(*cuts[s])
        slot = side - ja - 1
        y, x = here.line(*offsets(s, ja, kb))
        return remote(
            in1.at[y, x, :, cols],
            in2.at[slot, kb, :, cols],
            sem2.at[s, ja, kb, 0],
            sem2.at[s, side - ja if sending else ja, kb, 1],
            here.at(*offsets(s, ja, 0)),
        )

    def second_copy(s, kb, sending):
        cols = pl.ds(*cuts[s])
        return remote(
            sum2.at[kb, :, cols],
            in3.at[side - kb - 1, :, cols],
            sem3.at[s, kb, 0],
            sem3.at[s, side - kb if sending else kb, 1],
            here.at(*offsets(s, 0, kb)),
        )

    def depth_copy(s, jz, sending):
        cols = pl.ds(*cuts[s])
        return remote(
            sum3.at[lax.rem(here.z + jz, depth), :, cols],
            in4.at[depth - jz - 1, :, cols],
            sem4.at[s, jz, 0],
            sem4.at[s, depth - jz if sending else jz, 1],
            here.at(0, 0, jz),
        )

    def go(copy):
        copy.start()
        sends.append(copy)

    def wide(value):
        return value.astype(jnp.float32)

    def phase0(s):
        cols = pl.ds(*cuts[s])
        value = produce(s, cols)
        part[:, :, :, :, cols] = value.astype(jnp.bfloat16).reshape(
            side, side, 2, depth * rows, cuts[s][1]
        )
        go(core_copy(s))

    def phase1(s):
        cols = pl.ds(*cuts[s])
        core_copy(s).wait_recv()
        for a in list(range(1, side)) + [0]:
            for b in list(range(1, side)) + [0]:
                y, x = here.line(*offsets(s, a, b))
                total = wide(part[y, x, here.core, :, cols]) + wide(in1[y, x, :, cols])
                in1[y, x, :, cols] = total.astype(jnp.bfloat16)
                if a:
                    go(first_copy(s, a, b, True))

    def phase2(s):
        cols = pl.ds(*cuts[s])
        for b in list(range(1, side)) + [0]:
            y, x = here.line(*offsets(s, 0, b))
            total = wide(in1[y, x, :, cols])
            for a in range(1, side):
                first_copy(s, a, b, False).wait_recv()
                total = total + wide(in2[a - 1, b, :, cols])
            sum2[b, :, cols] = total.astype(jnp.bfloat16)
            if b:
                go(second_copy(s, b, True))

    def phase3(s):
        cols = pl.ds(*cuts[s])
        total = wide(sum2[0, :, cols])
        for b in range(1, side):
            second_copy(s, b, False).wait_recv()
            total = total + wide(in3[b - 1, :, cols])
        if depth == 1:
            finish(s, cols, total)
            return
        sum3[:, :, cols] = total.astype(jnp.bfloat16).reshape(depth, rows, cuts[s][1])
        for jz in range(1, depth):
            go(depth_copy(s, jz, True))

    def phase4(s):
        if depth == 1:
            return
        cols = pl.ds(*cuts[s])
        total = wide(sum3[here.z, :, cols])
        for jz in range(1, depth):
            depth_copy(s, jz, False).wait_recv()
            total = total + wide(in4[jz - 1, :, cols])
        finish(s, cols, total)

    phases = tuple(zip((phase0, phase1, phase2, phase3, phase4), lags))
    for step in range(len(cuts) + phases[-1][1]):
        for phase, lag in phases:
            if 0 <= step - lag < len(cuts):
                phase(step - lag)
    for copy in sends:
        copy.wait_send()


def plane_of(here):
    side = here.side
    return (
        [here.at(flip=True)]
        + [here.at(dy=j) for j in range(1, side)]
        + [here.at(dx=j) for j in range(1, side)]
    )


def projection_kernel(
    side, attended, weight_hbm, resid, gain, router, chosen, hidden, packed, weight, regrouped, part, wsem, ssem, rsem, *scratch
):
    here = Place(side, 1)
    rows = attended.shape[0]
    count = 2 * side * side
    width = attended.shape[1] // count
    z = lax.axis_index("dp")
    load = pltpu.make_async_copy(weight_hbm, weight, wsem)
    load.start()

    def peer(j):
        return lax.rem(here.ep + j, count)

    greet([(peer(j), z) for j in range(1, count)])

    def piece(index):
        return attended.at[:, pl.ds(pl.multiple_of(index * width, 128), width)]

    def exchange(j, sending):
        return remote(
            piece(peer(j)),
            regrouped.at[here.ep],
            ssem.at[j],
            rsem.at[count - j if sending else j],
            (peer(j), z),
        )

    for j in range(1, count):
        exchange(j, True).start()
    regrouped[here.ep] = attended[:, pl.ds(pl.multiple_of(here.ep * width, 128), width)]
    load.wait()
    for j in range(1, count):
        remote(
            piece(peer(j)), regrouped.at[peer(j)], ssem.at[j], rsem.at[j], (peer(j), z)
        ).wait_recv()

    def produce(s, cols):
        left = regrouped[...].reshape(count * rows, width)
        return jnp.dot(left, weight[:, cols], preferred_element_type=jnp.float32)

    def finish(s, cols, total):
        value = resid[:, cols].astype(jnp.float32) + total
        hidden[:, cols] = value
        squares.append(jnp.sum(value * value, axis=1, keepdims=True))

    squares = []

    reduce_scatter(here, rows, hidden.shape[1], produce, finish, (0, 2, 5, 8, 8), part, scratch)
    features = hidden.shape[1]
    scale = lax.rsqrt(jnp.maximum(sum(squares) / features, 0.25))
    logits = jnp.zeros((rows, router.shape[1]), jnp.float32)
    for start, size in slices_of(features):
        cols = pl.ds(start, size)
        normed = (hidden[:, cols] * scale * gain[:, cols]).astype(jnp.bfloat16)
        packed[:, cols] = normed
        logits = logits + jnp.dot(normed, router[cols, :], preferred_element_type=jnp.float32)
    named = chosen[...] > 0
    peak = jnp.max(jnp.where(named, logits, -jnp.inf), axis=1, keepdims=True)
    grown = jnp.where(named, jnp.exp(jnp.where(named, logits - peak, 0.0)), 0.0)
    probs = grown / jnp.sum(grown, axis=1, keepdims=True)
    packed[:, features:] = jnp.zeros((rows, packed.shape[1] - features), jnp.bfloat16)
    packed[:, features : features + router.shape[1]] = probs.astype(jnp.bfloat16)
    for j in range(1, count):
        exchange(j, True).wait_send()


def project(side, attended, out_proj, resid, gain, router, chosen):
    rows, width = resid.shape
    count = 2 * side * side
    dma = pltpu.SemaphoreType.DMA
    vmem = pl.BlockSpec(memory_space=pltpu.VMEM)
    return pl.pallas_call(
        lambda *refs: projection_kernel(side, *refs),
        out_shape=(
            jax.ShapeDtypeStruct((rows, width), jnp.float32),
            jax.ShapeDtypeStruct((rows, width + pl.cdiv(router.shape[1], 128) * 128), jnp.bfloat16),
        ),
        in_specs=[vmem, pl.BlockSpec(memory_space=pl.ANY), vmem, vmem, vmem, vmem],
        out_specs=(vmem, vmem),
        scratch_shapes=[
            pltpu.VMEM(out_proj.shape, jnp.bfloat16),
            pltpu.VMEM((count, rows, attended.shape[1] // count), jnp.bfloat16),
            pltpu.VMEM((side, side, 2, rows, width), jnp.bfloat16),
            dma(()),
            dma((count,)),
            dma((count,)),
        ]
        + reduce_shapes(side, 1, rows, width),
        compiler_params=pltpu.CompilerParams(
            collective_id=0, has_side_effects=True, vmem_limit_bytes=VMEM_LIMIT
        ),
    )(attended, out_proj, resid, gain, router, chosen)


def all_gather(here, own, held, consume, zsem, lsem, csem, send_sem, copy_sem):
    side, depth = here.side, here.depth
    width = D
    cuts = slices_of(width, own.shape[1] - width)
    sends = []
    rows = own.shape[0]

    def rows_of(z):
        return pl.ds(pl.multiple_of(z * rows, rows), rows)

    local_copy = pltpu.make_async_copy(own, held.at[here.y, here.x, here.core, rows_of(here.z)], copy_sem)
    local_copy.start()

    def go(copy):
        copy.start()
        sends.append(copy)

    def depth_copy(s, j, sending):
        cols = pl.ds(*cuts[s])
        z = here.z if sending else lax.rem(here.z + j, depth)
        return remote(
            own.at[:, cols],
            held.at[here.y, here.x, here.core, rows_of(z), cols],
            zsem.at[s, j, 0],
            zsem.at[s, depth - j if sending else j, 1],
            here.at(0, 0, j),
        )

    def line_ref(s, ky, kx, core):
        y, x = here.line(ky, kx)
        return held.at[y, x, core, :, pl.ds(*cuts[s])]

    def plane_send(s, ky, kx, jy, jx):
        ref = line_ref(s, ky, kx, here.core)
        go(
            remote(
                ref,
                ref,
                send_sem.at[s, ky, kx, jy, jx],
                lsem.at[s, (ky - jy) % side, (kx - jx) % side],
                here.at(jy, jx),
            )
        )

    def core_send(s, ky, kx):
        ref = line_ref(s, ky, kx, here.core)
        go(remote(ref, ref, csem.at[s, ky, kx, 0], csem.at[s, ky, kx, 1], here.at(flip=True)))

    def plane_wait(s, ky, kx):
        ref = line_ref(s, ky, kx, here.core)
        remote(ref, ref, send_sem.at[s, 0, 0, 0, 0], lsem.at[s, ky, kx], here.at(flip=True)).wait_recv()

    def core_wait(s, ky, kx):
        ref = line_ref(s, ky, kx, 1 - here.core)
        remote(ref, ref, csem.at[s, ky, kx, 0], csem.at[s, ky, kx, 1], here.at(flip=True)).wait_recv()

    def turn(s, a, b):
        return (a, b) if s % 2 == 0 else (b, a)

    def phase1(s):
        for j in range(1, depth):
            depth_copy(s, j, False).wait_recv()
        for j in range(1, side):
            plane_send(s, 0, 0, *turn(s, j, 0))
            plane_send(s, 0, 0, *turn(s, 0, j))
        core_send(s, 0, 0)

    def phase2(s):
        for k in range(1, side):
            plane_wait(s, *turn(s, k, 0))
            for j in range(1, side):
                plane_send(s, *turn(s, k, 0), *turn(s, 0, j))
            core_send(s, *turn(s, k, 0))

    def phase3(s):
        for b in range(1, side):
            for a in range(side):
                plane_wait(s, *turn(s, a, b))
                core_send(s, *turn(s, a, b))

    for s in range(len(cuts)):
        for j in range(1, depth):
            go(depth_copy(s, j, True))
    local_copy.wait()
    def phase4(s):
        for a in range(side):
            for b in range(side):
                core_wait(s, a, b)
        consume(s)

    phases = ((phase1, 0), (phase2, 2), (phase3, 4), (phase4, 5))
    for step in range(len(cuts) + phases[-1][1]):
        for phase, lag in phases:
            if 0 <= step - lag < len(cuts):
                phase(step - lag)
    for copy in sends:
        copy.wait_send()


def expert_kernel(
    side, depth, own, gate_hbm, up_hbm, down_hbm, mixed,
    gate, up, down, held, act, gate_sum, up_sum, wsem, zsem, lsem, csem, send_sem, copy_sem, *scratch
):
    here = Place(side, depth)
    rows = own.shape[0]
    loads = [
        pltpu.make_async_copy(src.at[0], dst, wsem.at[i])
        for i, (src, dst) in enumerate(((gate_hbm, gate), (up_hbm, up), (down_hbm, down)))
    ]
    for load in loads:
        load.start()
    greet(plane_of(here) + [here.at(0, 0, j) for j in range(1, depth)])
    group = side * 2 * depth * rows

    def rows_at(y):
        return pl.ds(pl.multiple_of(y * group, group), group)

    def consume(s):
        if s == 0:
            loads[0].wait()
            loads[1].wait()
        start = 512 * s

        def step(y, carry):
            block = held[y, :, :, :, start : start + 512].reshape(group, 512)
            for weight, total in ((gate, gate_sum), (up, up_sum)):
                value = jnp.dot(
                    block, weight[start : start + 512, :], preferred_element_type=jnp.float32
                )
                total[rows_at(y), :] = value if s == 0 else total[rows_at(y), :] + value
            return carry

        lax.fori_loop(0, side, step, 0)

    all_gather(here, own, held, consume, zsem, lsem, csem, send_sem, copy_sem)
    loads[2].wait()
    expert = (here.ep * depth + here.z) // 2

    def activate(y, carry):
        tail = held[y, :, :, :, D:].reshape(group, held.shape[-1] - D)
        lane = lax.broadcasted_iota(jnp.int32, tail.shape, 1)
        weight = jnp.sum(
            jnp.where(lane == expert, tail.astype(jnp.float32), 0.0), axis=1, keepdims=True
        )
        gate_val = gate_sum[rows_at(y), :]
        value = gate_val / (1.0 + jnp.exp(-gate_val)) * up_sum[rows_at(y), :] * weight
        act[rows_at(y), :] = value.astype(jnp.bfloat16)
        return carry

    lax.fori_loop(0, side, activate, 0)

    def produce(s, cols):
        return jnp.dot(act[...], down[:, cols], preferred_element_type=jnp.float32)

    def finish(s, cols, total):
        mixed[:, cols] = total

    reduce_scatter(here, rows, mixed.shape[1], produce, finish, (0, 1, 3, 5, 7), held, scratch)


def run_experts(side, depth, packed, gate_slab, up_slab, down_slab):
    rows, width = packed.shape[0], down_slab.shape[2]
    n = width // 512
    dma = pltpu.SemaphoreType.DMA
    count = 2 * side * side * depth
    vmem, anywhere = pl.BlockSpec(memory_space=pltpu.VMEM), pl.BlockSpec(memory_space=pl.ANY)
    return pl.pallas_call(
        lambda *refs: expert_kernel(side, depth, *refs),
        out_shape=jax.ShapeDtypeStruct((rows, width), jnp.float32),
        in_specs=[vmem, anywhere, anywhere, anywhere],
        out_specs=vmem,
        scratch_shapes=[
            pltpu.VMEM(gate_slab.shape[1:], jnp.bfloat16),
            pltpu.VMEM(up_slab.shape[1:], jnp.bfloat16),
            pltpu.VMEM(down_slab.shape[1:], jnp.bfloat16),
            pltpu.VMEM((side, side, 2, depth * rows, packed.shape[1]), jnp.bfloat16),
            pltpu.VMEM((count * rows, gate_slab.shape[2]), jnp.bfloat16),
            pltpu.VMEM((count * rows, gate_slab.shape[2]), jnp.float32),
            pltpu.VMEM((count * rows, gate_slab.shape[2]), jnp.float32),
            dma((3,)),
            dma((n, depth, 2)),
            dma((n, side, side)),
            dma((n, side, side, 2)),
            dma((n, side, side, side, side)),
            dma(()),
        ]
        + reduce_shapes(side, depth, rows, width),
        compiler_params=pltpu.CompilerParams(
            collective_id=1, has_side_effects=True, vmem_limit_bytes=VMEM_LIMIT
        ),
    )(packed, gate_slab, up_slab, down_slab)


def local(
    resid,
    queries,
    new_keys,
    new_values,
    cache_keys,
    cache_values,
    cache_len,
    out_proj,
    norm_gain,
    router,
    expert_ids,
    gate_slab,
    up_slab,
    down_slab,
):
    attended = attend(queries, new_keys, new_values, cache_keys, cache_values, cache_len)
    side = math.isqrt(lax.axis_size("ep") // 2)
    depth = lax.axis_size("dp")
    labels = jnp.arange(router.shape[1], dtype=jnp.int32)
    chosen = jnp.any(expert_ids[:, :, None] == labels[None, None, :], axis=1).astype(jnp.float32)
    hidden, packed = project(
        side, attended, out_proj, resid, norm_gain.reshape(1, -1), router, chosen
    )
    return hidden + run_experts(side, depth, packed, gate_slab, up_slab, down_slab)


def solution(mesh):
    in_specs = (
        P(("ep", "dp"), None),
        P(("ep", "dp"), None),
        P(("ep", "dp"), None),
        P(("ep", "dp"), None),
        P(("ep", "dp"), None, None),
        P(("ep", "dp"), None, None),
        P(("ep", "dp")),
        P("ep", None),
        P(),
        P(),
        P(("ep", "dp"), None),
        P(("ep", "dp"), None, None),
        P(("ep", "dp"), None, None),
        P(("ep", "dp"), None, None),
    )
    out_specs = P(("ep", "dp"), None)
    return jax.shard_map(local, mesh=mesh, in_specs=in_specs, out_specs=out_specs, check_vma=False)
```
